8 devices in a mesh: data: 2 (over z, y), tp: 4 (over x, core).
Axes of the slice: x: 2, y: 2, z: 1, core: 2. Of those that a mesh axis runs over, the one named last changes fastest.
Arguments:
- x: bfloat16 [2048, 49152], P('data', 'tp'), parts along dimension 0
- w: bfloat16 [49152, 12288], P('tp')
Outputs:
- output: bfloat16 [2048, 12288], P('data'), parts along dimension 0
There are 2 independent parts. The reference program is written for one: setup_inputs(seed, part) draws one part's arguments, and reference() takes and returns one part's arrays. A program takes and returns all parts, laid end to end along the dimension named above; an argument that names none is the same for every part.
All inputs are finite; a program needn't handle non-finite values.
Results may differ from the reference program's by a relative error of at most 0.0103027.
Values are sent between devices in bfloat16 or wider.
A program may use at most 1.5 GiB of HBM per device.

```python
import jax
import jax.numpy as jnp

TOKENS = 1024
D = 12288
FF = 49152


def setup_inputs(seed: int = 0, part: int = 0) -> dict:
    key = jax.random.key(seed)
    kx = jax.random.fold_in(jax.random.fold_in(key, 1), part)
    kw = jax.random.fold_in(key, 2)
    x = jax.random.normal(kx, (TOKENS, FF), jnp.float32)
    w = jax.random.normal(kw, (FF, D), jnp.float32) * (FF ** -0.5)
    return {"x": x.astype(jnp.bfloat16), "w": w.astype(jnp.bfloat16)}


def reference(x, w):
    y = jnp.dot(x, w, preferred_element_type=jnp.float32)
    return y.astype(jnp.bfloat16)
```

```python
import functools

import jax
import jax.numpy as jnp
from jax import lax
from jax.experimental import pallas as pl
from jax.experimental.pallas import tpu as pltpu
from jax.sharding import PartitionSpec as P

BF16, F32 = jnp.bfloat16, jnp.float32
NC = 512
BK = 2048
HR = 256
SLOTS = 6


def kernel(nb, nch, x_hbm, w_hbm, r_hbm, xv, wv, part, sb1, rb1, ch, rb2, yb,
           xsem, wsem, s1s, s1r, s2s, s2r, s4s, s4r, lsem):
    me = lax.axis_index("tp")
    core = lax.rem(me, 2)
    partner = me + 1 - 2 * core
    across = lax.rem(me + 2, 4)
    off = (pl.multiple_of((1 - core) * HR, HR),
           pl.multiple_of(core * HR, HR))

    def x_copy(p, h, b):
        row = pl.multiple_of(p * 2 * HR + off[h], HR)
        return pltpu.make_async_copy(
            x_hbm.at[pl.ds(row, HR), pl.ds(b * BK, BK)],
            xv.at[p, pl.ds(off[h], HR), pl.ds(b * BK, BK)], xsem.at[2 * p + h, b])

    def w_copy(n, b):
        col = pl.multiple_of(n * NC, NC)
        par = lax.rem(n, 2)
        return pltpu.make_async_copy(
            w_hbm.at[pl.ds(b * BK, BK), pl.ds(col, NC)],
            wv.at[par, pl.ds(b * BK, BK), :], wsem.at[par, b])

    def remote(src, dst, ssem, rsem, to):
        return pltpu.make_async_remote_copy(
            src_ref=src, dst_ref=dst, send_sem=ssem, recv_sem=rsem,
            device_id={"tp": to}, device_id_type=pl.DeviceIdType.MESH)

    def send1(u):
        p, s = lax.rem(u, 2), lax.rem(u, 4)
        return remote(sb1.at[p], rb1.at[s], s1s.at[p], s1r.at[s], partner)

    def send2(u):
        s = lax.rem(u, SLOTS)
        return remote(ch.at[s], rb2.at[s], s2s.at[s], s2r.at[s], across)

    def place(u):
        row = lax.rem(u, 2) * 2 * HR + core * HR
        return r_hbm.at[pl.ds(pl.multiple_of(row, HR), HR), pl.ds(pl.multiple_of(u // 2 * NC, NC), NC)]

    def send4(u, s):
        return remote(yb.at[s], place(u), s4s.at[s], s4r.at[lax.rem(u, 4)], partner)

    def keep4(u, s):
        return pltpu.make_async_copy(yb.at[s], place(u), lsem.at[s])

    def done(copy):
        copy.wait_recv()
        copy.wait_send()

    def start4(u, s):
        send4(u, s).start()
        keep4(u, s).start()

    def wait4(u, s):
        done(send4(u, s))
        keep4(u, s).wait()

    def dot(n, p, h, k0=0, k1=nb):
        return jnp.dot(xv[p, pl.ds(off[h], HR), pl.ds(k0 * BK, (k1 - k0) * BK)],
                       wv[lax.rem(n, 2), pl.ds(k0 * BK, (k1 - k0) * BK), :], preferred_element_type=F32)

    def theirs(n, p):
        sb1[p] = dot(n, p, 0).astype(BF16)

    def ours(n, p):
        u = 2 * n + p
        ch[lax.rem(u, SLOTS)] = (dot(n, p, 1) + rb1[lax.rem(u, 4)].astype(F32)).astype(BF16)

    def add2(u, s):
        slot = lax.rem(u + SLOTS, SLOTS)
        yb[s] = ch[slot] + rb2[slot]

    for b in range(nb):
        x_copy(0, 0, b).start()
        w_copy(0, b).start()
        x_copy(1, 0, b).start()
    for p in range(2):
        for b in range(nb):
            x_copy(p, 1, b).start()
    for b in range(nb):
        w_copy(1, b).start()

    barrier = pltpu.get_barrier_semaphore()
    for other in (partner, across):
        pl.semaphore_signal(barrier, inc=1, device_id={"tp": other},
                            device_id_type=pl.DeviceIdType.MESH)
    pl.semaphore_wait(barrier, 2)

    for b in range(nb):
        x_copy(0, 0, b).wait()
        w_copy(0, b).wait()
        x_copy(1, 0, b).wait()
        for p in range(2):
            d = dot(0, p, 0, b, b + 1)
            if b == 0:
                part[p] = d
            elif b < nb - 1:
                part[p] += d
            else:
                sb1[p] = (part[p] + d).astype(BF16)
    send1(0).start()

    @pl.loop(0, nch - 1)
    def _(n):
        u = 2 * n
        done(send1(u))
        send1(u + 1).start()

        @pl.when(n >= 2)
        def _():
            start4(u - 3, 1)

        @pl.when(n == 0)
        def _():
            for b in range(nb):
                x_copy(0, 1, b).wait()
        ours(n, 0)

        @pl.when(n >= 1)
        def _():
            done(send2(u - 2))
        send2(u).start()

        @pl.when(n >= 2)
        def _():
            wait4(u - 3, 1)
        for b in range(nb):
            w_copy(n + 1, b).wait()
        theirs(n + 1, 0)
        add2(u - 2, 0)

        done(send1(u + 1))
        send1(u + 2).start()

        @pl.when(n >= 1)
        def _():
            start4(u - 2, 0)

        @pl.when(n == 0)
        def _():
            for b in range(nb):
                x_copy(1, 1, b).wait()
        ours(n, 1)

        @pl.when(n >= 1)
        def _():
            done(send2(u - 1))
        send2(u + 1).start()

        @pl.when(n >= 1)
        def _():
            wait4(u - 2, 0)

        @pl.when(n < nch - 2)
        def _():
            for b in range(nb):
                w_copy(n + 2, b).start()
        theirs(n + 1, 1)
        add2(u - 1, 1)

    n, u = nch - 1, 2 * nch - 2
    done(send1(u))
    send1(u + 1).start()
    start4(u - 3, 1)
    ours(n, 0)
    done(send2(u - 2))
    send2(u).start()
    wait4(u - 3, 1)
    done(send1(u + 1))
    ours(n, 1)
    send2(u + 1).start()
    add2(u - 2, 0)
    start4(u - 2, 0)
    done(send2(u - 1))
    add2(u - 1, 1)
    start4(u - 1, 1)
    for v in (u, u + 1):
        s = v % 2
        wait4(v - 2, s)
        done(send2(v))
        add2(v, s)
        start4(v, s)
    for v in (u, u + 1):
        wait4(v, v % 2)


def solution(mesh):
    def local(x, w):
        rows, depth = x.shape
        cols = w.shape[1]
        nb, nch = depth // BK, cols // NC
        dma = pltpu.SemaphoreType.DMA
        return pl.pallas_call(
            functools.partial(kernel, nb, nch),
            out_shape=jax.ShapeDtypeStruct((rows, cols), BF16),
            in_specs=[pl.BlockSpec(memory_space=pl.ANY)] * 2,
            out_specs=pl.BlockSpec(memory_space=pl.ANY),
            scratch_shapes=[
                pltpu.VMEM((2, 2 * HR, depth), BF16),
                pltpu.VMEM((2, depth, NC), BF16),
                pltpu.VMEM((2, HR, NC), F32),
                pltpu.VMEM((2, HR, NC), BF16),
                pltpu.VMEM((4, HR, NC), BF16),
                pltpu.VMEM((SLOTS, HR, NC), BF16),
                pltpu.VMEM((SLOTS, HR, NC), BF16),
                pltpu.VMEM((2, HR, NC), BF16),
                dma((4, nb)), dma((2, nb)),
                dma((2,)), dma((4,)),
                dma((SLOTS,)), dma((SLOTS,)),
                dma((2,)), dma((4,)), dma((2,)),
            ],
            compiler_params=pltpu.CompilerParams(
                collective_id=0, has_side_effects=True, vmem_limit_bytes=63 * 1024 * 1024),
            cost_estimate=pl.CostEstimate(
                flops=2 * rows * depth * cols, transcendentals=0,
                bytes_accessed=2 * (rows * depth + depth * cols + rows * cols)),
            name="rowparallel",
        )(x, w)

    return jax.shard_map(local, mesh=mesh, in_specs=(P("data", "tp"), P("tp", None)),
                         out_specs=P("data", None), check_vma=False)
```

```python
import functools

import jax
import jax.numpy as jnp
from jax import lax
from jax.experimental import pallas as pl
from jax.experimental.pallas import tpu as pltpu
from jax.sharding import PartitionSpec as P

BF16, F32 = jnp.bfloat16, jnp.float32
NC = 256
BK = 2048
WS = 4
SLOTS = 6


def kernel(nb, nu, hr, x_hbm, w_hbm, r_hbm, xv, wv, part, sb1, rb1, ch, rb2, yb,
           xsem, wsem, s1s, s1r, s2s, s2r, s4s, s4r, lsem):
    me = lax.axis_index("tp")
    core = lax.rem(me, 2)
    partner = me + 1 - 2 * core
    across = lax.rem(me + 2, 4)
    off_o = pl.multiple_of((1 - core) * hr, hr)
    off_m = pl.multiple_of(core * hr, hr)

    def x_copy(b):
        return pltpu.make_async_copy(
            x_hbm.at[:, pl.ds(b * BK, BK)], xv.at[:, pl.ds(b * BK, BK)], xsem.at[b])

    def w_copy(u, b):
        col = pl.multiple_of(u * NC, NC)
        s = lax.rem(u, WS)
        return pltpu.make_async_copy(
            w_hbm.at[pl.ds(b * BK, BK), pl.ds(col, NC)],
            wv.at[s, pl.ds(b * BK, BK), :], wsem.at[s, b])

    def remote(src, dst, ssem, rsem, to):
        return pltpu.make_async_remote_copy(
            src_ref=src, dst_ref=dst, send_sem=ssem, recv_sem=rsem,
            device_id={"tp": to}, device_id_type=pl.DeviceIdType.MESH)

    def send1(u):
        p, s = lax.rem(u, 2), lax.rem(u, 4)
        return remote(sb1.at[p], rb1.at[s], s1s.at[p], s1r.at[s], partner)

    def send2(u):
        s = lax.rem(u, SLOTS)
        return remote(ch.at[s], rb2.at[s], s2s.at[s], s2r.at[s], across)

    def place(u):
        return r_hbm.at[pl.ds(off_m, hr), pl.ds(pl.multiple_of(u * NC, NC), NC)]

    def send4(u):
        p = lax.rem(u, 2)
        return remote(yb.at[p], place(u), s4s.at[p], s4r.at[lax.rem(u, 4)], partner)

    def keep4(u):
        p = lax.rem(u, 2)
        return pltpu.make_async_copy(yb.at[p], place(u), lsem.at[p])

    def done(copy):
        copy.wait_recv()
        copy.wait_send()

    def start4(u):
        send4(u).start()
        keep4(u).start()

    def wait4(u):
        done(send4(u))
        keep4(u).wait()

    def theirs(u, cuts=1):
        r = hr // cuts
        for c in range(cuts):
            sb1[lax.rem(u, 2), pl.ds(c * r, r), :] = jnp.dot(
                xv[pl.ds(off_o + c * r, r), :], wv[lax.rem(u, WS)], preferred_element_type=F32).astype(BF16)

    def ours(u, cuts=1):
        r = hr // cuts
        for c in range(cuts):
            ch[lax.rem(u, SLOTS), pl.ds(c * r, r), :] = (
                jnp.dot(xv[pl.ds(off_m + c * r, r), :], wv[lax.rem(u, WS)], preferred_element_type=F32)
                + rb1[lax.rem(u, 4), pl.ds(c * r, r), :].astype(F32)).astype(BF16)

    def add2(u):
        slot = lax.rem(u + SLOTS, SLOTS)
        yb[lax.rem(u + 2, 2)] = ch[slot] + rb2[slot]

    for b in range(nb):
        x_copy(b).start()
        w_copy(0, b).start()
        w_copy(1, b).start()
    for u in (2, 3):
        for b in range(nb):
            w_copy(u, b).start()

    barrier = pltpu.get_barrier_semaphore()
    for other in (partner, across):
        pl.semaphore_signal(barrier, inc=1, device_id={"tp": other},
                            device_id_type=pl.DeviceIdType.MESH)
    pl.semaphore_wait(barrier, 2)

    for b in range(nb):
        x_copy(b).wait()
        w_copy(0, b).wait()
        w_copy(1, b).wait()
        for u in range(2):
            d = jnp.dot(xv[:, pl.ds(b * BK, BK)], wv[u, pl.ds(b * BK, BK), :], preferred_element_type=F32)
            if b == 0:
                part[u] = d
            else:
                part[u] += d
    for u in range(2):
        sb1[u] = part[u, pl.ds(off_o, hr), :].astype(BF16)
    send1(0).start()
    send1(1).start()
    for b in range(nb):
        w_copy(4, b).start()
        w_copy(2, b).wait()
    done(send1(0))
    theirs(2, 2)
    done(send1(1))
    send1(2).start()
    for b in range(nb):
        w_copy(3, b).wait()
    theirs(3, 2)
    for u in range(2):
        ch[u] = (part[u, pl.ds(off_m, hr), :] + rb1[u].astype(F32)).astype(BF16)
    send2(0).start()

    @pl.loop(2, nu - 2)
    def _(u):
        done(send1(u))

        @pl.when(u >= 3)
        def _():
            done(send2(u - 3))

        @pl.when(u >= 5)
        def _():
            wait4(u - 5)
        send1(u + 1).start()
        send2(u - 1).start()

        @pl.when(u >= 4)
        def _():
            start4(u - 4)

        @pl.when(u < nu - 3)
        def _():
            for b in range(nb):
                w_copy(u + 3, b).start()
        for b in range(nb):
            w_copy(u + 2, b).wait()
        ours(u)
        theirs(u + 2)
        add2(u - 3)

    for u in (nu - 2, nu - 1):
        done(send1(u))
        done(send2(u - 3))
        wait4(u - 5)
        if u + 1 < nu:
            send1(u + 1).start()
        send2(u - 1).start()
        start4(u - 4)
        ours(u, 2)
        add2(u - 3)
    send2(nu - 1).start()
    start4(nu - 4)
    for u in range(nu - 3, nu):
        done(send2(u))
        wait4(u - 2)
        add2(u)
        start4(u)
    wait4(nu - 2)
    wait4(nu - 1)


CP = 32


def last_copy(r_hbm, y_hbm, buf, isem, osem):
    n = buf.shape[0]

    def into(i):
        return pltpu.make_async_copy(r_hbm.at[pl.ds(i * CP, CP), :], buf.at[i], isem.at[i])

    def out(i):
        return pltpu.make_async_copy(buf.at[i], y_hbm.at[pl.ds(i * CP, CP), :], osem.at[i])

    for i in range(n):
        into(i).start()
    for i in range(n):
        into(i).wait()
        out(i).start()
    for i in range(n):
        out(i).wait()


def solution(mesh):
    def local(x, w):
        rows, depth = x.shape
        cols = w.shape[1]
        nb, nu, hr = depth // BK, cols // NC, rows // 2
        dma = pltpu.SemaphoreType.DMA
        r = pl.pallas_call(
            functools.partial(kernel, nb, nu, hr),
            out_shape=jax.ShapeDtypeStruct((rows, cols), BF16),
            in_specs=[pl.BlockSpec(memory_space=pl.ANY)] * 2,
            out_specs=pl.BlockSpec(memory_space=pl.ANY),
            scratch_shapes=[
                pltpu.VMEM((rows, depth), BF16),
                pltpu.VMEM((WS, depth, NC), BF16),
                pltpu.VMEM((2, rows, NC), F32),
                pltpu.VMEM((2, hr, NC), BF16),
                pltpu.VMEM((4, hr, NC), BF16),
                pltpu.VMEM((SLOTS, hr, NC), BF16),
                pltpu.VMEM((SLOTS, hr, NC), BF16),
                pltpu.VMEM((2, hr, NC), BF16),
                dma((nb,)), dma((WS, nb)),
                dma((2,)), dma((4,)),
                dma((SLOTS,)), dma((SLOTS,)),
                dma((2,)), dma((4,)), dma((2,)),
            ],
            compiler_params=pltpu.CompilerParams(
                collective_id=0, has_side_effects=True, vmem_limit_bytes=63 * 1024 * 1024),
            cost_estimate=pl.CostEstimate(
                flops=2 * rows * depth * cols, transcendentals=0,
                bytes_accessed=2 * (rows * depth + depth * cols + rows * cols)),
            name="rowparallel",
        )(x, w)

        return pl.pallas_call(
            last_copy,
            out_shape=jax.ShapeDtypeStruct((rows, cols), BF16),
            in_specs=[pl.BlockSpec(memory_space=pl.ANY)],
            out_specs=pl.BlockSpec(memory_space=pl.ANY),
            scratch_shapes=[pltpu.VMEM((rows // CP, CP, cols), BF16), dma((rows // CP,)), dma((rows // CP,))],
            compiler_params=pltpu.CompilerParams(vmem_limit_bytes=63 * 1024 * 1024),
            name="lastcopy",
        )(r)

    return jax.shard_map(local, mesh=mesh, in_specs=(P("data", "tp"), P("tp", None)),
                         out_specs=P("data", None), check_vma=False)
```

```python
import functools

import jax
import jax.numpy as jnp
from jax import lax
from jax.experimental import pallas as pl
from jax.experimental.pallas import tpu as pltpu
from jax.sharding import PartitionSpec as P

BF16, F32 = jnp.bfloat16, jnp.float32
NC = 256
BK = 2048
WS = 4
SLOTS = 6


def kernel(nb, nu, hr, x_hbm, w_hbm, r_hbm, xv, wv, part, sb1, rb1, ch, rb2, yb,
           xsem, wsem, wusem, s1s, s1r, s2s, s2r, s4s, s4r, lsem):
    me = lax.axis_index("tp")
    core = lax.rem(me, 2)
    partner = me + 1 - 2 * core
    across = lax.rem(me + 2, 4)
    off_o = pl.multiple_of((1 - core) * hr, hr)
    off_m = pl.multiple_of(core * hr, hr)

    def x_copy(b):
        return pltpu.make_async_copy(
            x_hbm.at[:, pl.ds(b * BK, BK)], xv.at[:, pl.ds(b * BK, BK)], xsem.at[b])

    def w_copy(u, b):
        col = pl.multiple_of(u * NC, NC)
        s = lax.rem(u, WS)
        return pltpu.make_async_copy(
            w_hbm.at[pl.ds(b * BK, BK), pl.ds(col, NC)],
            wv.at[s, pl.ds(b * BK, BK), :], wsem.at[s, b])

    def w_unit(u):
        s = lax.rem(u, WS)
        return pltpu.make_async_copy(
            w_hbm.at[:, pl.ds(pl.multiple_of(u * NC, NC), NC)], wv.at[s], wusem.at[s])

    def remote(src, dst, ssem, rsem, to):
        return pltpu.make_async_remote_copy(
            src_ref=src, dst_ref=dst, send_sem=ssem, recv_sem=rsem,
            device_id={"tp": to}, device_id_type=pl.DeviceIdType.MESH)

    def send1(u):
        p, s = lax.rem(u, 2), lax.rem(u, 4)
        return remote(sb1.at[p], rb1.at[s], s1s.at[p], s1r.at[s], partner)

    def send2(u):
        s = lax.rem(u, SLOTS)
        return remote(ch.at[s], rb2.at[s], s2s.at[s], s2r.at[s], across)

    def place(u):
        return r_hbm.at[pl.ds(off_m, hr), pl.ds(pl.multiple_of(u * NC, NC), NC)]

    def send4(u):
        p = lax.rem(u, 2)
        return remote(yb.at[p], place(u), s4s.at[p], s4r, partner)

    def keep4(u):
        p = lax.rem(u, 2)
        return pltpu.make_async_copy(yb.at[p], place(u), lsem.at[p])

    def done(copy):
        copy.wait_recv()
        copy.wait_send()

    def start4(u):
        send4(u).start()
        keep4(u).start()

    def wait4(u):
        send4(u).wait_send()
        keep4(u).wait()

    def theirs(u, cuts=1):
        r = hr // cuts
        for c in range(cuts):
            sb1[lax.rem(u, 2), pl.ds(c * r, r), :] = jnp.dot(
                xv[pl.ds(off_o + c * r, r), :], wv[lax.rem(u, WS)], preferred_element_type=F32).astype(BF16)

    def ours(u, cuts=1):
        r = hr // cuts
        for c in range(cuts):
            ch[lax.rem(u, SLOTS), pl.ds(c * r, r), :] = (
                jnp.dot(xv[pl.ds(off_m + c * r, r), :], wv[lax.rem(u, WS)], preferred_element_type=F32)
                + rb1[lax.rem(u, 4), pl.ds(c * r, r), :].astype(F32)).astype(BF16)

    def add2(u):
        slot = lax.rem(u + SLOTS, SLOTS)
        yb[lax.rem(u + 2, 2)] = ch[slot] + rb2[slot]

    for b in range(nb):
        x_copy(b).start()
        w_copy(0, b).start()
        w_copy(1, b).start()
    for u in (2, 3):
        w_unit(u).start()

    barrier = pltpu.get_barrier_semaphore()
    for other in (partner, across):
        pl.semaphore_signal(barrier, inc=1, device_id={"tp": other},
                            device_id_type=pl.DeviceIdType.MESH)
    pl.semaphore_wait(barrier, 2)

    for b in range(nb):
        x_copy(b).wait()
        w_copy(0, b).wait()
        w_copy(1, b).wait()
        for u in range(2):
            d = jnp.dot(xv[:, pl.ds(b * BK, BK)], wv[u, pl.ds(b * BK, BK), :], preferred_element_type=F32)
            if b == 0:
                part[u] = d
            else:
                part[u] += d
    for u in range(2):
        sb1[u] = part[u, pl.ds(off_o, hr), :].astype(BF16)
    send1(0).start()
    send1(1).start()
    w_unit(4).start()
    w_unit(2).wait()
    done(send1(0))
    theirs(2, 2)
    done(send1(1))
    send1(2).start()
    w_unit(3).wait()
    theirs(3, 2)
    for u in range(2):
        ch[u] = (part[u, pl.ds(off_m, hr), :] + rb1[u].astype(F32)).astype(BF16)
    send2(0).start()

    @pl.loop(2, nu - 2)
    def _(u):
        done(send1(u))

        @pl.when(u >= 3)
        def _():
            done(send2(u - 3))

        @pl.when(u >= 5)
        def _():
            wait4(u - 5)
        send1(u + 1).start()
        send2(u - 1).start()

        @pl.when(u >= 4)
        def _():
            start4(u - 4)

        @pl.when(u < nu - 3)
        def _():
            w_unit(u + 3).start()
        w_unit(u + 2).wait()
        ours(u)
        theirs(u + 2)
        add2(u - 3)

    for u in (nu - 2, nu - 1):
        done(send1(u))
        done(send2(u - 3))
        wait4(u - 5)
        if u + 1 < nu:
            send1(u + 1).start()
        send2(u - 1).start()
        start4(u - 4)
        ours(u, 2)
        add2(u - 3)
    send2(nu - 1).start()
    start4(nu - 4)
    for u in range(nu - 3, nu):
        done(send2(u))
        wait4(u - 2)
        add2(u)
        start4(u)
    wait4(nu - 2)
    wait4(nu - 1)
    theirs_here = r_hbm.at[pl.ds(off_o, hr), :]
    pltpu.make_async_copy(theirs_here, theirs_here, s4r).wait()


CP = 32


def last_copy(r_hbm, y_hbm, buf, isem, osem):
    n = buf.shape[0]

    def into(i):
        return pltpu.make_async_copy(r_hbm.at[pl.ds(i * CP, CP), :], buf.at[i], isem.at[i])

    def out(i):
        return pltpu.make_async_copy(buf.at[i], y_hbm.at[pl.ds(i * CP, CP), :], osem.at[i])

    for i in range(n):
        into(i).start()
    for i in range(n):
        into(i).wait()
        out(i).start()
    for i in range(n):
        out(i).wait()


def solution(mesh):
    def local(x, w):
        rows, depth = x.shape
        cols = w.shape[1]
        nb, nu, hr = depth // BK, cols // NC, rows // 2
        dma = pltpu.SemaphoreType.DMA
        r = pl.pallas_call(
            functools.partial(kernel, nb, nu, hr),
            out_shape=jax.ShapeDtypeStruct((rows, cols), BF16),
            in_specs=[pl.BlockSpec(memory_space=pl.ANY)] * 2,
            out_specs=pl.BlockSpec(memory_space=pl.ANY),
            scratch_shapes=[
                pltpu.VMEM((rows, depth), BF16),
                pltpu.VMEM((WS, depth, NC), BF16),
                pltpu.VMEM((2, rows, NC), F32),
                pltpu.VMEM((2, hr, NC), BF16),
                pltpu.VMEM((4, hr, NC), BF16),
                pltpu.VMEM((SLOTS, hr, NC), BF16),
                pltpu.VMEM((SLOTS, hr, NC), BF16),
                pltpu.VMEM((2, hr, NC), BF16),
                dma((nb,)), dma((2, nb)), dma((WS,)),
                dma((2,)), dma((4,)),
                dma((SLOTS,)), dma((SLOTS,)),
                dma((2,)), dma(()), dma((2,)),
            ],
            compiler_params=pltpu.CompilerParams(
                collective_id=0, has_side_effects=True, vmem_limit_bytes=63 * 1024 * 1024),
            cost_estimate=pl.CostEstimate(
                flops=2 * rows * depth * cols, transcendentals=0,
                bytes_accessed=2 * (rows * depth + depth * cols + rows * cols)),
            name="rowparallel",
        )(x, w)

        return pl.pallas_call(
            last_copy,
            out_shape=jax.ShapeDtypeStruct((rows, cols), BF16),
            in_specs=[pl.BlockSpec(memory_space=pl.ANY)],
            out_specs=pl.BlockSpec(memory_space=pl.ANY),
            scratch_shapes=[pltpu.VMEM((rows // CP, CP, cols), BF16), dma((rows // CP,)), dma((rows // CP,))],
            compiler_params=pltpu.CompilerParams(vmem_limit_bytes=63 * 1024 * 1024),
            name="lastcopy",
        )(r)

    return jax.shard_map(local, mesh=mesh, in_specs=(P("data", "tp"), P("tp", None)),
                         out_specs=P("data", None), check_vma=False)
```

```python
import functools

import jax
import jax.numpy as jnp
from jax import lax
from jax.experimental import pallas as pl
from jax.experimental.pallas import tpu as pltpu
from jax.sharding import PartitionSpec as P

BF16, F32 = jnp.bfloat16, jnp.float32
NC = 256
BK = 2048
WS = 4
SLOTS = 6


def kernel(nb, nu, hr, x_hbm, w_hbm, r_hbm, c_hbm, xv, wv, part, sb1, rb1, ch, rb2, yb,
           xsem, wsem, wusem, s1s, s1r, s2s, s2r, s4s, s4r, lsem, csem):
    me = lax.axis_index("tp")
    core = lax.rem(me, 2)
    partner = me + 1 - 2 * core
    across = lax.rem(me + 2, 4)
    off_o = pl.multiple_of((1 - core) * hr, hr)
    off_m = pl.multiple_of(core * hr, hr)

    def x_copy(b):
        return pltpu.make_async_copy(
            x_hbm.at[:, pl.ds(b * BK, BK)], xv.at[:, pl.ds(b * BK, BK)], xsem.at[b])

    def w_copy(u, b):
        col = pl.multiple_of(u * NC, NC)
        s = lax.rem(u, WS)
        return pltpu.make_async_copy(
            w_hbm.at[pl.ds(b * BK, BK), pl.ds(col, NC)],
            wv.at[s, pl.ds(b * BK, BK), :], wsem.at[s, b])

    def w_unit(u):
        s = lax.rem(u, WS)
        return pltpu.make_async_copy(
            w_hbm.at[:, pl.ds(pl.multiple_of(u * NC, NC), NC)], wv.at[s], wusem.at[s])

    def remote(src, dst, ssem, rsem, to):
        return pltpu.make_async_remote_copy(
            src_ref=src, dst_ref=dst, send_sem=ssem, recv_sem=rsem,
            device_id={"tp": to}, device_id_type=pl.DeviceIdType.MESH)

    def send1(u):
        s = lax.rem(u, 4)
        return remote(sb1.at[s], rb1.at[s], s1s.at[s], s1r.at[s], partner)

    def send2(u):
        s = lax.rem(u, SLOTS)
        return remote(ch.at[s], rb2.at[s], s2s.at[s], s2r.at[s], across)

    def place(u):
        return r_hbm.at[pl.ds(off_m, hr), pl.ds(pl.multiple_of(u * NC, NC), NC)]

    def send4(u):
        p = lax.rem(u, 2)
        return remote(yb.at[p], place(u), s4s.at[p], s4r, partner)

    def keep4(u):
        p = lax.rem(u, 2)
        return pltpu.make_async_copy(yb.at[p], place(u), lsem.at[p])

    def keepc(i):
        return pltpu.make_async_copy(
            ch.at[(nu - 2 + i) % SLOTS], c_hbm.at[:, pl.ds(i * NC, NC)], csem.at[i])

    def done(copy):
        copy.wait_recv()
        copy.wait_send()

    def start4(u):
        send4(u).start()
        keep4(u).start()

    def wait4(u):
        send4(u).wait_send()
        keep4(u).wait()

    def theirs(u, cuts=1):
        r = hr // cuts
        for c in range(cuts):
            sb1[lax.rem(u, 4), pl.ds(c * r, r), :] = jnp.dot(
                xv[pl.ds(off_o + c * r, r), :], wv[lax.rem(u, WS)], preferred_element_type=F32).astype(BF16)

    def ours(u, cuts=1):
        r = hr // cuts
        for c in range(cuts):
            ch[lax.rem(u, SLOTS), pl.ds(c * r, r), :] = (
                jnp.dot(xv[pl.ds(off_m + c * r, r), :], wv[lax.rem(u, WS)], preferred_element_type=F32)
                + rb1[lax.rem(u, 4), pl.ds(c * r, r), :].astype(F32)).astype(BF16)

    def add2(u):
        slot = lax.rem(u + SLOTS, SLOTS)
        yb[lax.rem(u + 2, 2)] = ch[slot] + rb2[slot]

    for b in range(nb):
        x_copy(b).start()
        w_copy(0, b).start()
        w_copy(1, b).start()
    for u in (2, 3):
        w_unit(u).start()

    barrier = pltpu.get_barrier_semaphore()
    for other in (partner, across):
        pl.semaphore_signal(barrier, inc=1, device_id={"tp": other},
                            device_id_type=pl.DeviceIdType.MESH)
    pl.semaphore_wait(barrier, 2)

    for b in range(nb):
        x_copy(b).wait()
        w_copy(0, b).wait()
        w_copy(1, b).wait()
        for u in range(2):
            d = jnp.dot(xv[:, pl.ds(b * BK, BK)], wv[u, pl.ds(b * BK, BK), :], preferred_element_type=F32)
            if b == 0:
                part[u] = d
            else:
                part[u] += d
    for u in range(2):
        sb1[u] = part[u, pl.ds(off_o, hr), :].astype(BF16)
    send1(0).start()
    send1(1).start()
    w_unit(4).start()
    w_unit(2).wait()
    theirs(2, 2)
    send1(2).start()
    w_unit(3).wait()
    done(send1(0))
    done(send1(1))
    theirs(3, 2)
    for u in range(2):
        ch[u] = (part[u, pl.ds(off_m, hr), :] + rb1[u].astype(F32)).astype(BF16)
    send2(0).start()

    @pl.loop(2, nu - 2)
    def _(u):
        done(send1(u))

        @pl.when(u >= 3)
        def _():
            done(send2(u - 3))

        @pl.when(u >= 5)
        def _():
            wait4(u - 5)
        send1(u + 1).start()
        send2(u - 1).start()

        @pl.when(u >= 4)
        def _():
            start4(u - 4)

        @pl.when(u < nu - 3)
        def _():
            w_unit(u + 3).start()
        w_unit(u + 2).wait()
        ours(u)
        theirs(u + 2)
        add2(u - 3)

    for u in (nu - 2, nu - 1):
        done(send1(u))
        done(send2(u - 3))
        wait4(u - 5)
        if u == nu - 2:
            send1(u + 1).start()
            send2(u - 1).start()
        else:
            keepc(0).start()
        start4(u - 4)
        ours(u, 2)
        add2(u - 3)
    keepc(1).start()
    start4(nu - 4)
    done(send2(nu - 3))
    wait4(nu - 5)
    add2(nu - 3)
    start4(nu - 3)
    wait4(nu - 4)
    wait4(nu - 3)
    keepc(0).wait()
    keepc(1).wait()
    theirs_here = r_hbm.at[pl.ds(off_o, hr), pl.ds(0, (nu - 2) * NC)]
    pltpu.make_async_copy(theirs_here, theirs_here, s4r).wait()


CP = 32


def last_copy(cols, r_hbm, y_hbm, buf, isem, osem):
    n = buf.shape[0]

    def into(i):
        return pltpu.make_async_copy(r_hbm.at[pl.ds(i * CP, CP), pl.ds(0, cols)], buf.at[i], isem.at[i])

    def out(i):
        return pltpu.make_async_copy(buf.at[i], y_hbm.at[pl.ds(i * CP, CP), pl.ds(0, cols)], osem.at[i])

    for i in range(n):
        into(i).start()
    for i in range(n):
        into(i).wait()
        out(i).start()
    for i in range(n):
        out(i).wait()


def last_units(y_in, mine, other, y_hbm, sem):
    core = lax.rem(lax.axis_index("tp"), 2)
    hr, width = mine.shape
    first = y_hbm.shape[1] - width
    outs = [pltpu.make_async_copy(
        src, y_hbm.at[pl.ds(pl.multiple_of(row * hr, hr), hr), pl.ds(first, width)], sem.at[i])
        for i, (src, row) in enumerate(((mine, core), (other, 1 - core)))]
    for c in outs:
        c.start()
    for c in outs:
        c.wait()


def solution(mesh):
    def local(x, w):
        rows, depth = x.shape
        cols = w.shape[1]
        nb, nu, hr = depth // BK, cols // NC, rows // 2
        dma, hbm = pltpu.SemaphoreType.DMA, pl.BlockSpec(memory_space=pl.ANY)
        r, c = pl.pallas_call(
            functools.partial(kernel, nb, nu, hr),
            out_shape=[jax.ShapeDtypeStruct((rows, cols), BF16), jax.ShapeDtypeStruct((hr, 2 * NC), BF16)],
            in_specs=[hbm] * 2,
            out_specs=[hbm] * 2,
            scratch_shapes=[
                pltpu.VMEM((rows, depth), BF16),
                pltpu.VMEM((WS, depth, NC), BF16),
                pltpu.VMEM((2, rows, NC), F32),
                pltpu.VMEM((4, hr, NC), BF16),
                pltpu.VMEM((4, hr, NC), BF16),
                pltpu.VMEM((SLOTS, hr, NC), BF16),
                pltpu.VMEM((SLOTS, hr, NC), BF16),
                pltpu.VMEM((2, hr, NC), BF16),
                dma((nb,)), dma((2, nb)), dma((WS,)),
                dma((4,)), dma((4,)),
                dma((SLOTS,)), dma((SLOTS,)),
                dma((2,)), dma(()), dma((2,)), dma((2,)),
            ],
            compiler_params=pltpu.CompilerParams(
                collective_id=0, has_side_effects=True, vmem_limit_bytes=63 * 1024 * 1024),
            cost_estimate=pl.CostEstimate(
                flops=2 * rows * depth * cols, transcendentals=0,
                bytes_accessed=2 * (rows * depth + depth * cols + rows * cols)),
            name="rowparallel",
        )(x, w)

        across = lax.ppermute(c, "tp", [(i, (i + 2) % 4) for i in range(4)])
        done = cols - 2 * NC
        y = pl.pallas_call(
            functools.partial(last_copy, done),
            out_shape=jax.ShapeDtypeStruct((rows, cols), BF16),
            in_specs=[hbm], out_specs=hbm,
            scratch_shapes=[pltpu.VMEM((rows // CP, CP, done), BF16), dma((rows // CP,)), dma((rows // CP,))],
            compiler_params=pltpu.CompilerParams(vmem_limit_bytes=63 * 1024 * 1024),
            cost_estimate=pl.CostEstimate(flops=0, transcendentals=0, bytes_accessed=4 * rows * done),
            name="lastcopy",
        )(r)
        across, y = lax.optimization_barrier((across, y))
        mine = c + across
        other = lax.ppermute(mine, "tp", [(0, 1), (1, 0), (2, 3), (3, 2)])
        return pl.pallas_call(
            last_units,
            out_shape=jax.ShapeDtypeStruct((rows, cols), BF16),
            in_specs=[hbm] + [pl.BlockSpec(memory_space=pltpu.VMEM)] * 2, out_specs=hbm,
            input_output_aliases={0: 0},
            scratch_shapes=[dma((2,))],
            name="lastunits",
        )(y, mine, other)

    return jax.shard_map(local, mesh=mesh, in_specs=(P("data", "tp"), P("tp", None)),
                         out_specs=P("data", None), check_vma=False)
```
